32 devices in a mesh: rep: 4 (over z), inst: 8 (over y, x, core).
Axes of the slice: x: 2, y: 2, z: 4, core: 2. Of those that a mesh axis runs over, the one named last changes fastest.
Arguments:
- acts: bfloat16 [32768, 4096], P(('rep', 'inst')), may hold values from -6 to 6
- grad_keys: bfloat16 [32768, 1024], P(('rep', 'inst')), may hold values from -0.0625 to 0.0625
- grad_values: bfloat16 [32768, 1024], P(('rep', 'inst')), may hold values from -0.0625 to 0.0625
- grad_logits: bfloat16 [8, 32768], P(None, ('rep', 'inst')), may hold values from -0.0625 to 0.0625
- order: int32 [32], replicated, may hold values from 0 to 31, each once
- bucket_param: float32 [4, 2048, 1024], P(None, 'inst'), may hold values from -6 to 6
- bucket_m: float32 [4, 2048, 1024], P(None, 'inst'), may hold values from -6 to 6
- bucket_v: float32 [4, 2048, 1024], P(None, 'inst'), may hold values from 0.25 to 4
- router_param: float32 [32, 1024], P('inst'), may hold values from -6 to 6
- router_m: float32 [32, 1024], P('inst'), may hold values from -6 to 6
- router_v: float32 [32, 1024], P('inst'), may hold values from 0.25 to 4
Outputs:
- new_param: float32 [4, 2048, 1024], P(None, 'inst')
- new_moment: float32 [4, 2048, 1024], P(None, 'inst')
- new_second: float32 [4, 2048, 1024], P(None, 'inst')
- router_new_param: float32 [32, 1024], P('inst')
- router_new_moment: float32 [32, 1024], P('inst')
- router_new_second: float32 [32, 1024], P('inst')
The draws below stay inside these ranges and needn't reach their ends.
Inputs may be any that keep to these rules, and one draw needn't show every extreme that they name: order is a permutation of the 32 row blocks; entries with k * 8 <= s < (k + 1) * 8 fill bucket k.
All inputs are finite; a program needn't handle non-finite values.
Results may differ from the reference program's by a relative error of at most 0.0003.
Values sent between devices are 32-bit elements; how exact they have to be, the bound alone decides.
A program may use at most 256 MiB of HBM per device.

```python
import math
import jax
import jax.numpy as jnp
from jax import lax

D = 4096
KV = 1024
EXPERTS = 8
BUCKETS = 4
BLOCK_ROWS = 256
TOKENS = 32768
BLOCKS = 32
BUCKET_ROWS = 2048
ROUTER_ROWS = 32


def levels(rng, extent, split, least, high):
    factor_of, own = 1.0, jax.random.fold_in(rng, 6)
    for axis_at, parts in split:
        steps = jnp.exp(jax.random.uniform(jax.random.fold_in(own, axis_at), (parts,), jnp.float32, least / len(split), high / len(split)))
        factor_of = factor_of * jnp.repeat(steps, extent[axis_at] // parts).reshape([-1 if axis == axis_at else 1 for axis in range(len(extent))])
    return factor_of


def centred(own_key, dims, spread, most, shards=(), dtype=jnp.bfloat16):
    entries = spread * jax.random.normal(own_key, dims, jnp.float32)
    if shards:
        entries = entries * levels(own_key, dims, shards, -0.22, 0.18)
    return jnp.clip(entries, -most, most).astype(dtype)


def setup_inputs(seed: int = 0) -> dict:
    arg_keys = jax.random.split(jax.random.key(seed), 12)
    acts = centred(arg_keys[0], (TOKENS, D), 1.0, 6.0, ((0, 32),))
    grad_keys = centred(arg_keys[1], (TOKENS, KV), (TOKENS // 4) ** -0.5, 0.0625, ((0, 32),))
    grad_values = centred(arg_keys[2], (TOKENS, KV), (TOKENS // 4) ** -0.5, 0.0625, ((0, 32),))
    grad_logits = centred(arg_keys[3], (EXPERTS, TOKENS), (TOKENS // 4) ** -0.5, 0.0625, ((1, 32),))
    order = jax.random.permutation(arg_keys[4], BLOCKS).astype(jnp.int32)
    bucket_param = centred(arg_keys[5], (BUCKETS, BUCKET_ROWS, KV), 1.0, 6.0, ((1, 8),), jnp.float32)
    bucket_m = centred(arg_keys[6], (BUCKETS, BUCKET_ROWS, KV), 1.0, 6.0, ((1, 8),), jnp.float32)
    bucket_v = jnp.clip(jnp.exp(math.log(4.0) - 2.7725887 * jax.random.uniform(arg_keys[7], (BUCKETS, BUCKET_ROWS, KV), jnp.float32) ** levels(arg_keys[7], (BUCKETS, BUCKET_ROWS, KV), ((1, 8),), -0.2, 0.2)), 0.25, 4.0)
    router_param = centred(arg_keys[8], (ROUTER_ROWS, KV), 1.0, 6.0, ((0, 8),), jnp.float32)
    router_m = centred(arg_keys[9], (ROUTER_ROWS, KV), 1.0, 6.0, ((0, 8),), jnp.float32)
    router_v = jnp.clip(jnp.exp(math.log(4.0) - 2.7725887 * jax.random.uniform(arg_keys[10], (ROUTER_ROWS, KV), jnp.float32) ** levels(arg_keys[10], (ROUTER_ROWS, KV), ((0, 8),), -0.2, 0.2)), 0.25, 4.0)
    return {"acts": acts, "grad_keys": grad_keys, "grad_values": grad_values, "grad_logits": grad_logits, "order": order, "bucket_param": bucket_param, "bucket_m": bucket_m, "bucket_v": bucket_v, "router_param": router_param, "router_m": router_m, "router_v": router_v}


beta_first = 0.9
beta_second = 0.95
step_rate = 0.05
decay_rate = 0.1
epsilon = 1e-08
correct_first = 1.0 - 0.9 ** 10
correct_second = 1.0 - 0.95 ** 10

def contract(left, right):
    return lax.dot_general(left, right, (((0,), (0,)), ((), ())), preferred_element_type=jnp.float32)

def adamw(grad, param, moment, second):
    moment_new = beta_first * moment + (1.0 - beta_first) * grad
    second_new = beta_second * second + (1.0 - beta_second) * grad * grad
    ratio = moment_new / correct_first / (jnp.sqrt(second_new / correct_second) + epsilon)
    param_new = param - step_rate * (ratio + decay_rate * param)
    return (param_new, moment_new, second_new)

def reference(acts, grad_keys, grad_values, grad_logits, order, bucket_param, bucket_m, bucket_v, router_param, router_m, router_v):
    weight_rows = jnp.concatenate([contract(acts, grad_keys), contract(acts, grad_values)], axis=0)
    blocks = weight_rows.reshape(BLOCKS, BLOCK_ROWS, KV)
    packed = jnp.take(blocks, order.astype(jnp.int32), axis=0).reshape(BUCKETS, BUCKET_ROWS, KV)
    router_grad = jnp.dot(grad_logits, acts, preferred_element_type=jnp.float32).reshape(ROUTER_ROWS, KV)
    new_param, new_moment, new_second = adamw(packed, bucket_param, bucket_m, bucket_v)
    router_new_param, router_new_moment, router_new_second = adamw(router_grad, router_param, router_m, router_v)
    return (new_param, new_moment, new_second, router_new_param, router_new_moment, router_new_second)
```

```python
import functools

import jax
import jax.numpy as jnp
from jax import lax
from jax.experimental import pallas as pl
from jax.experimental.pallas import tpu as pltpu
from jax.sharding import PartitionSpec as P

MESH = pl.DeviceIdType.MESH
BUCKETS = 4
BLOCK_ROWS = 256
COLS = 128
LAG = 2


beta_first = 0.9
beta_second = 0.95
step_rate = 0.05
decay_rate = 0.1
epsilon = 1e-08
correct_first = 1.0 - 0.9**10
correct_second = 1.0 - 0.95**10


def adamw(grad, param, moment, second):
    moment_new = beta_first * moment + (1.0 - beta_first) * grad
    second_new = beta_second * second + (1.0 - beta_second) * grad * grad
    ratio = moment_new / correct_first / (jnp.sqrt(second_new / correct_second) + epsilon)
    param_new = param - step_rate * (ratio + decay_rate * param)
    return (param_new, moment_new, second_new)


def when_between(p, count, body):
    @pl.when(jnp.logical_and(p >= 0, p < count))
    def _():
        body(p)


class Lane:
    def __init__(self, n_inst, n_rep, dims, root, parts, send, recv, halves, lefts, rights, finish):
        self.n_inst, self.n_rep, self.dims, self.root = n_inst, n_rep, dims, root
        self.parts, self.send, self.recv = parts, send, recv
        self.halves, self.lefts, self.rights, self.finish = halves, lefts, rights, finish
        self.me = lax.axis_index("inst")
        self.rep = lax.axis_index("rep")
        self.stages = len(dims)
        self.base = 1 + LAG * (self.stages - 1)
        self.top = self.base + LAG * max(root, n_rep - 1 - root)

    def partner(self, bit):
        return self.me + (1 - 2 * ((self.me // 2**bit) % 2)) * 2**bit

    def owner(self, q):
        index = self.me
        for at, bit in enumerate(self.dims):
            if (q >> (self.stages - 1 - at)) & 1:
                index = index + (1 - 2 * ((self.me // 2**bit) % 2)) * 2**bit
        return index

    def copy(self, src, dst, stage, p, **device):
        return pltpu.make_async_remote_copy(
            src_ref=src,
            dst_ref=dst,
            send_sem=self.send.at[stage, p],
            recv_sem=self.recv.at[stage, p],
            device_id=device,
            device_id_type=MESH,
        )

    def half_copy(self, stage, p):
        count = self.n_inst >> (stage + 1)
        source = self.parts(p) if stage == 0 else self.halves(stage - 1, p)
        return self.copy(
            source.at[pl.ds(count, count)],
            self.halves(stage, p),
            stage,
            p,
            inst=self.partner(self.dims[stage]),
        )

    def add_half(self, stage, p):
        self.half_copy(stage, p).wait()
        count = self.n_inst >> (stage + 1)
        source = self.parts(p) if stage == 0 else self.halves(stage - 1, p)
        into = self.halves(stage, p)
        into[...] += source[pl.ds(0, count)]

    def total(self, p):
        return self.halves(self.stages - 1, p)

    def to_right(self, src, p):
        return self.copy(src, self.lefts(p), self.stages, p, rep=self.rep + 1)

    def to_left(self, src, p):
        return self.copy(src, self.rights(p), self.stages + 1, p, rep=self.rep - 1)

    def reduce_ends(self, p):
        if self.root > 0:

            @pl.when(self.rep == 0)
            def _():
                self.to_right(self.total(p), p).start()

        if self.root < self.n_rep - 1:

            @pl.when(self.rep == self.n_rep - 1)
            def _():
                self.to_left(self.total(p), p).start()

    def from_left(self, p):
        self.to_right(self.total(p), p).wait_recv()

    def from_right(self, p):
        self.to_left(self.total(p), p).wait_recv()

    def reduce_inner(self, t, count):
        rep, root, last = self.rep, self.root, self.n_rep - 1
        if root > 1:
            p = t - self.base - LAG * rep

            @pl.when((rep > 0) & (rep < root) & (p >= 0) & (p < count))
            def _():
                self.from_left(p)
                total = self.total(p)
                total[...] += self.lefts(p)[...]
                self.to_right(total, p).start()

        if root < last - 1:
            p2 = t - self.base - LAG * (last - rep)

            @pl.when((rep > root) & (rep < last) & (p2 >= 0) & (p2 < count))
            def _():
                self.from_right(p2)
                total = self.total(p2)
                total[...] += self.rights(p2)[...]
                self.to_left(total, p2).start()

    def at_root(self, t, count):
        p = t - self.top

        @pl.when((self.rep == self.root) & (p >= 0) & (p < count))
        def _():
            total = self.total(p)
            if self.root > 0:
                self.from_left(p)
                total[...] += self.lefts(p)[...]
            if self.root < self.n_rep - 1:
                self.from_right(p)
                total[...] += self.rights(p)[...]
            if self.root > 0:
                self.to_left(total, p).start()
            if self.root < self.n_rep - 1:
                self.to_right(total, p).start()
            self.finish(total, p)

    def spread(self, t, count):
        rep, root, last = self.rep, self.root, self.n_rep - 1
        if root > 0:
            p = t - self.top - LAG * (root - rep)

            @pl.when((rep < root) & (p >= 0) & (p < count))
            def _():
                self.from_right(p)
                if root > 1:

                    @pl.when(rep > 0)
                    def _():
                        self.to_left(self.rights(p), p).start()

                self.finish(self.rights(p), p)

        if root < last:
            p2 = t - self.top - LAG * (rep - root)

            @pl.when((rep > root) & (p2 >= 0) & (p2 < count))
            def _():
                self.from_left(p2)
                if root < last - 1:

                    @pl.when(rep < last)
                    def _():
                        self.to_right(self.lefts(p2), p2).start()

                self.finish(self.lefts(p2), p2)

    def settle(self, p):
        @pl.when(self.rep < self.n_rep - 1)
        def _():
            self.to_right(self.total(p), p).wait_send()

        @pl.when(self.rep > 0)
        def _():
            self.to_left(self.total(p), p).wait_send()

    def last_step(self):
        return self.top + LAG * max(self.root, self.n_rep - 1 - self.root)


def kernel(
    n_inst,
    n_rep,
    order,
    acts,
    keys,
    values,
    logits,
    out,
    router_out,
    slabs,
    turned,
    router_all,
    parts,
    router_parts,
    load,
    *scratch,
):
    bits = n_inst.bit_length() - 1
    rows = parts.shape[-1]
    width = router_parts.shape[-1]
    per_bucket = order.shape[0] // BUCKETS
    column_blocks = acts.shape[1] // BLOCK_ROWS
    chunks = keys.shape[1] // COLS
    count = chunks * BUCKETS // 2
    halves = scratch[:bits]
    router_halves = scratch[bits : 2 * bits]
    lefts, rights, router_lefts, router_rights = scratch[2 * bits : 2 * bits + 4]
    sends, recvs, router_sends, router_recvs = scratch[2 * bits + 4 :]

    def finish(kind):
        def body(ref, p):
            bucket = 2 * (p // chunks) + kind
            start = pl.multiple_of((p % chunks) * COLS, COLS)
            out[bucket, :, pl.ds(start, COLS)] = ref[0].T

        return body

    def router_finish(ref, p):
        router_out[...] = ref[0]

    forward = [0] + list(range(1, bits))
    backward = [0] + list(range(bits - 1, 0, -1))
    lanes = []
    for kind, dims in enumerate((forward, backward)):
        lanes.append(
            Lane(
                n_inst,
                n_rep,
                dims,
                ((n_rep - 1) // 2, n_rep // 2)[kind],
                lambda p, kind=kind: parts.at[kind, p % 2],
                sends.at[kind],
                recvs.at[kind],
                lambda stage, p, kind=kind: halves[stage].at[kind, p],
                lambda p, kind=kind: lefts.at[kind, p],
                lambda p, kind=kind: rights.at[kind, p],
                finish(kind),
            )
        )
    router = Lane(
        n_inst,
        n_rep,
        forward,
        (n_rep - 1) // 2,
        lambda p: router_parts,
        router_sends,
        router_recvs,
        lambda stage, p: router_halves[stage],
        lambda p: router_lefts,
        lambda p: router_rights,
        router_finish,
    )
    me, rep = lax.axis_index("inst"), lax.axis_index("rep")

    loads = [
        pltpu.make_async_copy(acts.at[:, pl.ds(at * rows, rows)], slabs.at[at], load.at[at])
        for at in range(slabs.shape[0])
    ]
    for copy in loads:
        copy.start()

    barrier = pltpu.get_barrier_semaphore()
    for bit in range(bits):
        pl.semaphore_signal(
            barrier, inc=1, device_id={"inst": router.partner(bit)}, device_id_type=MESH
        )

    @pl.when(rep > 0)
    def _():
        pl.semaphore_signal(barrier, inc=1, device_id={"rep": rep - 1}, device_id_type=MESH)

    @pl.when(rep < n_rep - 1)
    def _():
        pl.semaphore_signal(barrier, inc=1, device_id={"rep": rep + 1}, device_id_type=MESH)

    ends = jnp.where(rep > 0, 1, 0) + jnp.where(rep < n_rep - 1, 1, 0)
    pl.semaphore_wait(barrier, bits + ends)
    for copy in loads:
        copy.wait()

    def products(p):
        start = pl.multiple_of((p % chunks) * COLS, COLS)
        turned[0] = keys[:, pl.ds(start, COLS)].T
        turned[1] = values[:, pl.ds(start, COLS)].T
        for kind, lane in enumerate(lanes):
            bucket = 2 * (p // chunks) + kind
            for q in reversed(range(n_inst)):
                first = lane.owner(q) * rows
                block = order[bucket * per_bucket + first // BLOCK_ROWS]
                at = lax.rem(block, column_blocks) * (BLOCK_ROWS // rows) + first % BLOCK_ROWS // rows
                parts[kind, p % 2, q] = jnp.dot(
                    turned[lax.div(block, column_blocks)],
                    slabs[at],
                    preferred_element_type=jnp.float32,
                )
            lane.half_copy(0, p).start()

    def router_products(p):
        for at in range(slabs.shape[0]):
            router_all[:, pl.ds(at * rows, rows)] = jnp.dot(
                logits[...], slabs[at], preferred_element_type=jnp.float32
            )
        for q in range(n_inst):
            first = router.owner(q) * width
            router_parts[q] = router_all[
                pl.ds(first // acts.shape[1], 1),
                pl.ds(pl.multiple_of(first % acts.shape[1], width), width),
            ]
        router.half_copy(0, 0).start()

    both = [(lane, count) for lane in lanes] + [(router, 1)]

    def step(t, carry):
        when_between(t, count, products)
        when_between(t, 1, router_products)
        for stage in range(bits):
            lag = 1 + LAG * stage
            for lane, most in both:

                def body(p, lane=lane, stage=stage):
                    lane.add_half(stage, p)
                    if stage < bits - 1:
                        lane.half_copy(stage + 1, p).start()
                    else:
                        lane.reduce_ends(p)

                when_between(t - lag, most, body)
        for lane, most in both:
            lane.reduce_inner(t, most)
            lane.at_root(t, most)
            lane.spread(t, most)
        return carry

    steps = count + max(lane.last_step() for lane, _ in both)
    lax.fori_loop(0, steps, step, 0)

    def close(p, carry):
        for lane in lanes:
            lane.settle(p)
        return carry

    lax.fori_loop(0, count, close, 0)
    router.settle(0)


def summed(order, acts, keys, values, logits, n_inst, n_rep, bucket_rows, router_size):
    bits = n_inst.bit_length() - 1
    rows = bucket_rows // n_inst
    width = router_size // n_inst
    kv = keys.shape[1]
    count = kv // COLS * BUCKETS // 2
    vmem = pl.BlockSpec(memory_space=pltpu.VMEM)
    f32 = jnp.float32
    scratch = [
        pltpu.VMEM((acts.shape[1] // rows, acts.shape[0], rows), acts.dtype),
        pltpu.VMEM((2, COLS, acts.shape[0]), acts.dtype),
        pltpu.VMEM((logits.shape[0], acts.shape[1]), f32),
        pltpu.VMEM((2, 2, n_inst, COLS, rows), f32),
        pltpu.VMEM((n_inst, 1, width), f32),
        pltpu.SemaphoreType.DMA((acts.shape[1] // rows,)),
    ]
    scratch += [pltpu.VMEM((2, count, n_inst >> (s + 1), COLS, rows), f32) for s in range(bits)]
    scratch += [pltpu.VMEM((n_inst >> (s + 1), 1, width), f32) for s in range(bits)]
    scratch += [pltpu.VMEM((2, count, 1, COLS, rows), f32)] * 2
    scratch += [pltpu.VMEM((1, 1, width), f32)] * 2
    scratch += [pltpu.SemaphoreType.DMA((2, bits + 2, count))] * 2
    scratch += [pltpu.SemaphoreType.DMA((bits + 2, 1))] * 2
    return pl.pallas_call(
        functools.partial(kernel, n_inst, n_rep),
        out_shape=(
            jax.ShapeDtypeStruct((BUCKETS, rows, kv), f32),
            jax.ShapeDtypeStruct((1, width), f32),
        ),
        in_specs=[
            pl.BlockSpec(memory_space=pltpu.SMEM),
            pl.BlockSpec(memory_space=pl.ANY),
            vmem,
            vmem,
            vmem,
        ],
        out_specs=(vmem, vmem),
        scratch_shapes=scratch,
        compiler_params=pltpu.CompilerParams(
            collective_id=0, has_side_effects=True, vmem_limit_bytes=67043328
        ),
        cost_estimate=pl.CostEstimate(
            flops=4 * acts.shape[0] * acts.shape[1] * kv,
            bytes_accessed=16 * 2**20,
            transcendentals=0,
        ),
    )(order, acts, keys, values, logits)


def on_device(
    n_inst,
    n_rep,
    acts,
    grad_keys,
    grad_values,
    grad_logits,
    order,
    bucket_param,
    bucket_m,
    bucket_v,
    router_param,
    router_m,
    router_v,
):
    total, router_total = summed(
        order,
        acts,
        grad_keys,
        grad_values,
        grad_logits,
        n_inst,
        n_rep,
        bucket_param.shape[1] * n_inst,
        router_param.size * n_inst,
    )
    fresh = adamw(total, bucket_param, bucket_m, bucket_v)
    router_fresh = adamw(router_total.reshape(router_param.shape), router_param, router_m, router_v)
    return fresh + router_fresh


def solution(mesh):
    return jax.shard_map(
        functools.partial(on_device, mesh.shape["inst"], mesh.shape["rep"]),
        mesh=mesh,
        in_specs=(
            P(("rep", "inst"), None),
            P(("rep", "inst"), None),
            P(("rep", "inst"), None),
            P(None, ("rep", "inst")),
            P(),
            P(None, "inst", None),
            P(None, "inst", None),
            P(None, "inst", None),
            P("inst", None),
            P("inst", None),
            P("inst", None),
        ),
        out_specs=(
            P(None, "inst", None),
            P(None, "inst", None),
            P(None, "inst", None),
            P("inst", None),
            P("inst", None),
            P("inst", None),
        ),
        check_vma=False,
    )
```

```python
import functools

import jax
import jax.numpy as jnp
from jax import lax
from jax.experimental import pallas as pl
from jax.experimental.pallas import tpu as pltpu
from jax.sharding import PartitionSpec as P

MESH = pl.DeviceIdType.MESH
BUCKETS = 4
BLOCK_ROWS = 256
COLS = 128
LAG = 1
SPLIT = 2


beta_first = 0.9
beta_second = 0.95
step_rate = 0.05
decay_rate = 0.1
epsilon = 1e-08
correct_first = 1.0 - 0.9**10
correct_second = 1.0 - 0.95**10


def adamw(grad, param, moment, second):
    moment_new = beta_first * moment + (1.0 - beta_first) * grad
    second_new = beta_second * second + (1.0 - beta_second) * grad * grad
    ratio = moment_new / correct_first / (jnp.sqrt(second_new / correct_second) + epsilon)
    param_new = param - step_rate * (ratio + decay_rate * param)
    return (param_new, moment_new, second_new)


def when_between(p, count, body):
    @pl.when(jnp.logical_and(p >= 0, p < count))
    def _():
        body(p)


class Lane:
    def __init__(self, n_inst, n_rep, dims, parts, send, recv, halves, lefts, rights, finish):
        self.n_inst, self.n_rep, self.dims = n_inst, n_rep, dims
        self.parts, self.send, self.recv = parts, send, recv
        self.halves, self.lefts, self.rights, self.finish = halves, lefts, rights, finish
        self.me = lax.axis_index("inst")
        self.rep = lax.axis_index("rep")
        self.stages = len(dims)
        self.base = 1 + LAG * (self.stages - 1)
        self.left = n_rep // 2 - 1
        self.top = self.base + LAG * (self.left + 1)

    def partner(self, bit):
        return self.me + (1 - 2 * ((self.me // 2**bit) % 2)) * 2**bit

    def owner(self, q):
        index = self.me
        for at, bit in enumerate(self.dims):
            if (q >> (self.stages - 1 - at)) & 1:
                index = index + (1 - 2 * ((self.me // 2**bit) % 2)) * 2**bit
        return index

    def copy(self, src, dst, stage, p, **device):
        return pltpu.make_async_remote_copy(
            src_ref=src,
            dst_ref=dst,
            send_sem=self.send.at[stage, p],
            recv_sem=self.recv.at[stage, p],
            device_id=device,
            device_id_type=MESH,
        )

    def half_copy(self, stage, p):
        count = self.n_inst >> (stage + 1)
        source = self.parts(p) if stage == 0 else self.halves(stage - 1, p)
        return self.copy(
            source.at[pl.ds(count, count)],
            self.halves(stage, p),
            stage,
            p,
            inst=self.partner(self.dims[stage]),
        )

    def add_half(self, stage, p):
        self.half_copy(stage, p).wait()
        count = self.n_inst >> (stage + 1)
        source = self.parts(p) if stage == 0 else self.halves(stage - 1, p)
        into = self.halves(stage, p)
        into[...] += source[pl.ds(0, count)]

    def total(self, p):
        return self.halves(self.stages - 1, p)

    def to_right(self, src, p):
        return self.copy(src, self.lefts(p), self.stages, p, rep=self.rep + 1)

    def to_left(self, src, p):
        return self.copy(src, self.rights(p), self.stages + 1, p, rep=self.rep - 1)

    def reduce_ends(self, p):
        if self.left > 0:

            @pl.when(self.rep == 0)
            def _():
                self.to_right(self.total(p), p).start()

            @pl.when(self.rep == self.n_rep - 1)
            def _():
                self.to_left(self.total(p), p).start()

    def from_left(self, p):
        self.to_right(self.total(p), p).wait_recv()

    def from_right(self, p):
        self.to_left(self.total(p), p).wait_recv()

    def reduce(self, t, count):
        rep, last = self.rep, self.n_rep - 1

        def towards_right(p):
            total = self.total(p)
            if self.left > 0:
                self.from_left(p)
                total[...] += self.lefts(p)[...]
            self.to_right(total, p).start()

        def towards_left(p):
            total = self.total(p)
            if self.left > 0:
                self.from_right(p)
                total[...] += self.rights(p)[...]
            self.to_left(total, p).start()

        first = min(1, self.left)
        p = t - self.base - LAG * rep

        @pl.when((rep >= first) & (rep <= self.left) & (p >= 0) & (p < count))
        def _():
            towards_right(p)

        p2 = t - self.base - LAG * (last - rep)

        @pl.when((rep > self.left) & (rep <= last - first) & (p2 >= 0) & (p2 < count))
        def _():
            towards_left(p2)

    def spread(self, t, count):
        rep, left, last = self.rep, self.left, self.n_rep - 1
        p = t - self.top - LAG * (left - rep)

        @pl.when((rep <= left) & (p >= 0) & (p < count))
        def _():
            self.from_right(p)
            whole = self.rights(p)

            @pl.when(rep == left)
            def _():
                whole[...] += self.total(p)[...]

            if left > 0:

                @pl.when(rep > 0)
                def _():
                    self.to_left(whole, p).start()

            self.finish(whole, p)

        p2 = t - self.top - LAG * (rep - left - 1)

        @pl.when((rep > left) & (p2 >= 0) & (p2 < count))
        def _():
            self.from_left(p2)
            whole = self.lefts(p2)

            @pl.when(rep == left + 1)
            def _():
                whole[...] += self.total(p2)[...]

            if left > 0:

                @pl.when(rep < last)
                def _():
                    self.to_right(whole, p2).start()

            self.finish(whole, p2)

    def settle(self, p):
        @pl.when(self.rep < self.n_rep - 1)
        def _():
            self.to_right(self.total(p), p).wait_send()

        @pl.when(self.rep > 0)
        def _():
            self.to_left(self.total(p), p).wait_send()

    def last_step(self):
        return self.top + LAG * self.left


def kernel(
    n_inst,
    n_rep,
    order,
    acts,
    keys,
    values,
    logits,
    out,
    router_out,
    slabs,
    turned,
    router_all,
    parts,
    router_parts,
    load,
    *scratch,
):
    bits = n_inst.bit_length() - 1
    rows = slabs.shape[-1]
    short = parts.shape[-1]
    width = router_parts.shape[-1]
    per_bucket = order.shape[0] // BUCKETS
    column_blocks = acts.shape[1] // BLOCK_ROWS
    chunks = keys.shape[1] // COLS
    split = rows // parts.shape[-1]
    count = chunks * split * BUCKETS // 2
    halves = scratch[:bits]
    router_halves = scratch[bits : 2 * bits]
    lefts, rights, router_lefts, router_rights = scratch[2 * bits : 2 * bits + 4]
    sends, recvs, router_sends, router_recvs = scratch[2 * bits + 4 :]

    def finish(kind):
        def body(ref, p):
            chunk = p // split
            bucket = 2 * (chunk // chunks) + kind
            start = pl.multiple_of((chunk % chunks) * COLS, COLS)
            top = pl.multiple_of((p % split) * short, short)
            out[bucket, pl.ds(top, short), pl.ds(start, COLS)] = ref[0].T

        return body

    def router_finish(ref, p):
        router_out[...] = ref[0]

    forward = [0] + list(range(1, bits))
    backward = [0] + list(range(bits - 1, 0, -1))
    lanes = []
    for kind, dims in enumerate((forward, backward)):
        lanes.append(
            Lane(
                n_inst,
                n_rep,
                dims,
                lambda p, kind=kind: parts.at[kind, p % (2 * split)],
                sends.at[kind],
                recvs.at[kind],
                lambda stage, p, kind=kind: halves[stage].at[kind, p],
                lambda p, kind=kind: lefts.at[kind, p],
                lambda p, kind=kind: rights.at[kind, p],
                finish(kind),
            )
        )
    router = Lane(
        n_inst,
        n_rep,
        forward,
        lambda p: router_parts,
        router_sends,
        router_recvs,
        lambda stage, p: router_halves[stage],
        lambda p: router_lefts,
        lambda p: router_rights,
        router_finish,
    )
    me, rep = lax.axis_index("inst"), lax.axis_index("rep")

    loads = [
        pltpu.make_async_copy(acts.at[:, pl.ds(at * rows, rows)], slabs.at[at], load.at[at])
        for at in range(slabs.shape[0])
    ]
    for copy in loads:
        copy.start()

    barrier = pltpu.get_barrier_semaphore()
    for bit in range(bits):
        pl.semaphore_signal(
            barrier, inc=1, device_id={"inst": router.partner(bit)}, device_id_type=MESH
        )

    @pl.when(rep > 0)
    def _():
        pl.semaphore_signal(barrier, inc=1, device_id={"rep": rep - 1}, device_id_type=MESH)

    @pl.when(rep < n_rep - 1)
    def _():
        pl.semaphore_signal(barrier, inc=1, device_id={"rep": rep + 1}, device_id_type=MESH)

    ends = jnp.where(rep > 0, 1, 0) + jnp.where(rep < n_rep - 1, 1, 0)
    pl.semaphore_wait(barrier, bits + ends)
    for copy in loads:
        copy.wait()

    def products(chunk):
        start = pl.multiple_of((chunk % chunks) * COLS, COLS)
        turned[0] = keys[:, pl.ds(start, COLS)].T
        turned[1] = values[:, pl.ds(start, COLS)].T
        for kind, lane in enumerate(lanes):
            bucket = 2 * (chunk // chunks) + kind
            for q in reversed(range(n_inst)):
                first = lane.owner(q) * rows
                block = order[bucket * per_bucket + first // BLOCK_ROWS]
                at = lax.rem(block, column_blocks) * (BLOCK_ROWS // rows) + first % BLOCK_ROWS // rows
                full = jnp.dot(
                    turned[lax.div(block, column_blocks)],
                    slabs[at],
                    preferred_element_type=jnp.float32,
                )
                for part in range(split):
                    slot = (chunk % 2) * split + part
                    parts[kind, slot, q] = full[:, part * short : (part + 1) * short]
            for part in range(split):
                lane.half_copy(0, chunk * split + part).start()

    def router_products(p):
        for at in range(slabs.shape[0]):
            router_all[:, pl.ds(at * rows, rows)] = jnp.dot(
                logits[...], slabs[at], preferred_element_type=jnp.float32
            )
        for q in range(n_inst):
            first = router.owner(q) * width
            router_parts[q] = router_all[
                pl.ds(first // acts.shape[1], 1),
                pl.ds(pl.multiple_of(first % acts.shape[1], width), width),
            ]
        router.half_copy(0, 0).start()

    both = [(lane, count) for lane in lanes] + [(router, 1)]

    def step(t, carry):
        @pl.when((t % split == 0) & (t < count))
        def _():
            products(t // split)

        when_between(t, 1, router_products)
        for stage in range(bits):
            lag = 1 + LAG * stage
            for lane, most in both:

                def body(p, lane=lane, stage=stage):
                    lane.add_half(stage, p)
                    if stage < bits - 1:
                        lane.half_copy(stage + 1, p).start()
                    else:
                        lane.reduce_ends(p)

                when_between(t - lag, most, body)
        for lane, most in both:
            lane.reduce(t, most)
            lane.spread(t, most)
        return carry

    steps = count + max(lane.last_step() for lane, _ in both)
    lax.fori_loop(0, steps, step, 0)

    def close(p, carry):
        for lane in lanes:
            lane.settle(p)
        return carry

    lax.fori_loop(0, count, close, 0)
    router.settle(0)


def summed(order, acts, keys, values, logits, n_inst, n_rep, bucket_rows, router_size):
    bits = n_inst.bit_length() - 1
    rows = bucket_rows // n_inst
    width = router_size // n_inst
    kv = keys.shape[1]
    split = max(1, min(SPLIT, rows // 128))
    short = rows // split
    count = kv // COLS * split * BUCKETS // 2
    vmem = pl.BlockSpec(memory_space=pltpu.VMEM)
    f32 = jnp.float32
    scratch = [
        pltpu.VMEM((acts.shape[1] // rows, acts.shape[0], rows), acts.dtype),
        pltpu.VMEM((2, COLS, acts.shape[0]), acts.dtype),
        pltpu.VMEM((logits.shape[0], acts.shape[1]), f32),
        pltpu.VMEM((2, 2 * split, n_inst, COLS, short), f32),
        pltpu.VMEM((n_inst, 1, width), f32),
        pltpu.SemaphoreType.DMA((acts.shape[1] // rows,)),
    ]
    scratch += [pltpu.VMEM((2, count, n_inst >> (s + 1), COLS, short), f32) for s in range(bits)]
    scratch += [pltpu.VMEM((n_inst >> (s + 1), 1, width), f32) for s in range(bits)]
    scratch += [pltpu.VMEM((2, count, 1, COLS, short), f32)] * 2
    scratch += [pltpu.VMEM((1, 1, width), f32)] * 2
    scratch += [pltpu.SemaphoreType.DMA((2, bits + 2, count))] * 2
    scratch += [pltpu.SemaphoreType.DMA((bits + 2, 1))] * 2
    return pl.pallas_call(
        functools.partial(kernel, n_inst, n_rep),
        out_shape=(
            jax.ShapeDtypeStruct((BUCKETS, rows, kv), f32),
            jax.ShapeDtypeStruct((1, width), f32),
        ),
        in_specs=[
            pl.BlockSpec(memory_space=pltpu.SMEM),
            pl.BlockSpec(memory_space=pl.ANY),
            vmem,
            vmem,
            vmem,
        ],
        out_specs=(vmem, vmem),
        scratch_shapes=scratch,
        compiler_params=pltpu.CompilerParams(
            collective_id=0, has_side_effects=True, vmem_limit_bytes=67043328
        ),
        cost_estimate=pl.CostEstimate(
            flops=4 * acts.shape[0] * acts.shape[1] * kv,
            bytes_accessed=16 * 2**20,
            transcendentals=0,
        ),
    )(order, acts, keys, values, logits)


def on_device(
    n_inst,
    n_rep,
    acts,
    grad_keys,
    grad_values,
    grad_logits,
    order,
    bucket_param,
    bucket_m,
    bucket_v,
    router_param,
    router_m,
    router_v,
):
    total, router_total = summed(
        order,
        acts,
        grad_keys,
        grad_values,
        grad_logits,
        n_inst,
        n_rep,
        bucket_param.shape[1] * n_inst,
        router_param.size * n_inst,
    )
    fresh = adamw(total, bucket_param, bucket_m, bucket_v)
    router_fresh = adamw(router_total.reshape(router_param.shape), router_param, router_m, router_v)
    return fresh + router_fresh


def solution(mesh):
    return jax.shard_map(
        functools.partial(on_device, mesh.shape["inst"], mesh.shape["rep"]),
        mesh=mesh,
        in_specs=(
            P(("rep", "inst"), None),
            P(("rep", "inst"), None),
            P(("rep", "inst"), None),
            P(None, ("rep", "inst")),
            P(),
            P(None, "inst", None),
            P(None, "inst", None),
            P(None, "inst", None),
            P("inst", None),
            P("inst", None),
            P("inst", None),
        ),
        out_specs=(
            P(None, "inst", None),
            P(None, "inst", None),
            P(None, "inst", None),
            P("inst", None),
            P("inst", None),
            P("inst", None),
        ),
        check_vma=False,
    )
```
